32 devices in a mesh: wide: 8 (over y, x, core), narrow: 4 (over z).
Axes of the slice: x: 2, y: 2, z: 4, core: 2. Of those that a mesh axis runs over, the one named last changes fastest.
Arguments:
- hamiltonian: float32 [64, 3, 128, 128], P(('wide', 'narrow')), may hold values from -3.3 to 3.3, as said below
- old_density: float32 [64, 3, 128, 128], P(('wide', 'narrow')), may hold values from -2 to 2
- neighbours: int32 [64, 3], P(('wide', 'narrow')), may hold values from 0 to 7, as said below
- live: int32 [64], P(('wide', 'narrow')), may hold values from 0 to 1, as said below
- potential: float32 [1], replicated, may hold values from -1 to 1
Outputs:
- density: float32 [64, 3, 128, 128], P(('wide', 'narrow'))
The draws below stay inside these ranges and needn't reach their ends.
Inputs may be any that keep to these rules, and one draw needn't show every extreme that they name: Within each cluster of 8 consecutive blocks, entry 0 is the block's own index in the cluster and entries 1 and 2 are its neighbours on a cycle through all blocks of the cluster: block a is entry 1 of its entry-2 neighbour and entry 2 of its entry-1 neighbour. Along the cycle the 2 blocks of one device stand next to each other in some order; the devices of the narrow axis follow each other in an order drawn from the seed. For each index of the narrow axis, the devices at wide indices i and i + 4 own at most 2 live blocks together; in every draw some device owns 2 live blocks. `hamiltonian`: the block Hamiltonian is symmetric: tile 1 of block c is the transpose of tile 2 of prev(c), and tile 0 is symmetric.
All inputs are finite; a program needn't handle non-finite values. Where the reference program divides by a largest or mean magnitude, that divisor is 1e-20 or more.
Results may differ from the reference program's by a relative error of at most 0.0001.
Values sent between devices are 32-bit elements; how exact they have to be, the bound alone decides.
No kernel may reach another device: no remote copies, remote signals or barrier semaphores. Data moves between devices by JAX's collectives and lax.ppermute only.
A program may use at most 64 MiB of HBM per device.

```python
import jax
import jax.numpy as jnp
from jax import lax

BLK = 128
SUB = 3
BLK_DEV = 2
ITERS = 4
NC = 8
NBLK = 64


coupling = 0.03


def device_order(owner_key):
    owners = NC // BLK_DEV
    half = owners // 2
    shuffled = jax.random.permutation(owner_key, owners).astype(jnp.int32)
    slots = jnp.arange(owners, dtype=jnp.int32)
    first_pos = jnp.sum(jnp.where(shuffled == 0, slots, 0)).astype(jnp.int32)
    half_pos = jnp.sum(jnp.where(shuffled == half, slots, 0)).astype(jnp.int32)
    after_pos = ((first_pos + 1) % owners).astype(jnp.int32)
    after_value = shuffled[after_pos]
    swapped = jnp.where(slots == after_pos, half, shuffled)
    swapped = jnp.where((slots == half_pos) & (half_pos != after_pos), after_value, swapped)
    return swapped.astype(jnp.int32)


def cycle_lists(key):
    clusters = NBLK // NC
    owners = NC // BLK_DEV
    order_keys = jax.random.split(jax.random.fold_in(key, 11), clusters * owners)

    def owner_order(owner_key):
        return jax.random.permutation(owner_key, BLK_DEV)
    within = jax.vmap(owner_order)(order_keys).astype(jnp.int32).reshape((clusters, owners, BLK_DEV))
    seq_keys = jax.random.split(jax.random.fold_in(key, 17), clusters)
    sequence = jax.vmap(device_order)(seq_keys).astype(jnp.int32)
    orders = (sequence[:, :, None] * BLK_DEV + within).reshape((clusters, NC)).astype(jnp.int32)
    flip = jax.random.randint(jax.random.fold_in(key, 13), (clusters, 1), 0, 2)
    orders = jnp.where(flip == 1, orders[:, ::-1], orders).astype(jnp.int32)
    position = jnp.argsort(orders, axis=1, stable=True).astype(jnp.int32)
    before = jnp.take_along_axis(orders, (position - 1) % NC, axis=1)
    behind = jnp.take_along_axis(orders, (position + 1) % NC, axis=1)
    itself = jnp.broadcast_to(jnp.arange(NC, dtype=jnp.int32)[None, :], position.shape)
    return jnp.stack([itself, before, behind], axis=-1).reshape((NBLK, 3)).astype(jnp.int32)


def draw_neighbours(key, part):
    return cycle_lists(key)


def draw_hamiltonian(key, part):
    local_ids = cycle_lists(key)
    cluster_start = jnp.arange(NBLK, dtype=jnp.int32) // NC * NC
    global_ids = local_ids + cluster_start[:, None]
    tile_key = jax.random.fold_in(key, 23)
    energy_key = jax.random.fold_in(key, 29)
    shape = (NBLK, SUB, BLK, BLK)
    random_tiles = jax.random.truncated_normal(tile_key, -4.0, 4.0, shape, jnp.float32) * coupling
    energies = jax.random.uniform(energy_key, (NBLK, BLK), jnp.float32, -2.5, 2.5)
    mirror_slot = jnp.array([0, 2, 1], dtype=jnp.int32)
    mirrored = random_tiles[global_ids, mirror_slot[None, :]]
    tiles = random_tiles + jnp.swapaxes(mirrored, -1, -2)
    onsite_add = energies[:, :, None] * jnp.eye(BLK, dtype=jnp.float32)[None, :, :]
    tiles = tiles.at[:, 0].add(onsite_add)
    return tiles.astype(jnp.float32)


def draw_live(key, part):
    narrow_count = NC // BLK_DEV
    wide_count = NBLK // NC
    half_count = wide_count // 2
    pair_kind = jax.random.randint(jax.random.fold_in(key, 31), (half_count * narrow_count,), 0, 6)
    forced_pair = jax.random.randint(jax.random.fold_in(key, 37), (), 0, half_count * narrow_count)
    forced_kind = jax.random.randint(jax.random.fold_in(key, 41), (), 0, 2)
    pair_kind = jnp.where(jnp.arange(half_count * narrow_count) == forced_pair, forced_kind, pair_kind)
    pair_kind = pair_kind.reshape((half_count, narrow_count))
    lower_table = jnp.array([2, 0, 1, 1, 0, 0], dtype=jnp.int32)
    upper_table = jnp.array([0, 2, 1, 0, 1, 0], dtype=jnp.int32)
    counts = jnp.concatenate([lower_table[pair_kind], upper_table[pair_kind]], axis=0)
    chosen_slot = jax.random.randint(jax.random.fold_in(key, 43), (wide_count, narrow_count), 0, 2)
    first_live = (counts == 2) | (counts == 1) & (chosen_slot == 0)
    second_live = (counts == 2) | (counts == 1) & (chosen_slot == 1)
    return jnp.stack([first_live, second_live], axis=-1).reshape((NBLK,)).astype(jnp.int32)


def steps_of(rng, shape, pieces, low, high):
    loudness = 1.0
    for dim, blocks in pieces:
        heights = jax.random.uniform(jax.random.fold_in(jax.random.fold_in(rng, 6), dim), (blocks,), jnp.float32, low / len(pieces), high / len(pieces))
        loudness = loudness * jnp.repeat(jnp.exp(heights), shape[dim] // blocks).reshape((-1,) + (1,) * (len(shape) - 1 - dim))
    return loudness


def scatter_about(own_key, dims, deviation, most, shards=(), held_as=jnp.bfloat16):
    entries = deviation * jax.random.normal(own_key, dims, jnp.float32)
    if shards:
        entries = entries * steps_of(own_key, dims, shards, -0.22, 0.18)
    return jnp.clip(entries, -most, most).astype(held_as)


def setup_inputs(seed: int = 0) -> dict:
    key_list = jax.random.split(jax.random.key(seed), 6)
    hamiltonian = draw_hamiltonian(jax.random.fold_in(key_list[5], 71), 0)
    old_density = scatter_about(key_list[1], (NBLK, SUB, BLK, BLK), 0.3, 2.0, ((0, 32),), jnp.float32)
    neighbours = draw_neighbours(jax.random.fold_in(key_list[5], 71), 0)
    live = draw_live(jax.random.fold_in(key_list[5], 71), 0)
    potential = jnp.clip(jax.random.uniform(key_list[4], (1,), jnp.float32, -1.0, 1.0), -1.0, 1.0)
    return dict(hamiltonian=hamiltonian, old_density=old_density, neighbours=neighbours, live=live, potential=potential)


epsilon = 1e-6


def product(left, right):
    return jnp.matmul(left, right, precision=lax.Precision.HIGHEST)


def transpose_tiles(tiles):
    return jnp.swapaxes(tiles, -1, -2)


def assemble(row_tiles, prev_onsite, next_onsite, level):
    zero_tile = jnp.zeros_like(prev_onsite)
    upper_rows = jnp.concatenate([row_tiles[..., 0, :, :], row_tiles[..., 1, :, :], row_tiles[..., 2, :, :]], axis=-1)
    middle_rows = jnp.concatenate([transpose_tiles(row_tiles[..., 1, :, :]), prev_onsite, zero_tile], axis=-1)
    lower_rows = jnp.concatenate([transpose_tiles(row_tiles[..., 2, :, :]), zero_tile, next_onsite], axis=-1)
    matrix = jnp.concatenate([upper_rows, middle_rows, lower_rows], axis=-2)
    order = matrix.shape[-1]
    return matrix - level * jnp.eye(order, dtype=matrix.dtype)


def sign_columns(matrix):
    order = matrix.shape[-1]
    width = order // SUB
    identity = jnp.eye(order, dtype=matrix.dtype)
    bound = jnp.max(jnp.sum(jnp.abs(matrix), axis=-1), axis=-1) + epsilon
    current = matrix / bound
    for sweep in range(ITERS):
        square = product(current, current)
        current = 0.5 * product(current, 3.0 * identity - square)
    columns = 0.5 * (identity[:, :width] - current[:, :width])
    return columns.reshape((SUB, width, width))


def reference(hamiltonian, old_density, neighbours, live, potential):
    level = potential[0]
    cluster_start = (jnp.arange(NBLK, dtype=jnp.int32) // NC * NC).astype(jnp.int32)
    global_ids = (neighbours + cluster_start[:, None]).astype(jnp.int32)
    onsite = hamiltonian[:, 0]

    def solve_block(block_index):
        row_tiles = hamiltonian[block_index]
        prev_onsite = onsite[global_ids[block_index, 1]]
        next_onsite = onsite[global_ids[block_index, 2]]
        return sign_columns(assemble(row_tiles, prev_onsite, next_onsite, level))

    computed = lax.map(solve_block, jnp.arange(NBLK, dtype=jnp.int32))
    fresh_cols = jnp.where(live[:, None, None, None] == 1, computed, old_density)
    from_prev = fresh_cols[global_ids[:, 1], 2]
    from_next = fresh_cols[global_ids[:, 2], 1]
    return jnp.stack([
        0.5 * (fresh_cols[:, 0] + transpose_tiles(fresh_cols[:, 0])),
        0.5 * (fresh_cols[:, 1] + transpose_tiles(from_prev)),
        0.5 * (fresh_cols[:, 2] + transpose_tiles(from_next)),
    ], axis=1)
```

```python
import functools

import jax
import jax.numpy as jnp
from jax import lax
from jax.experimental import pallas as pl
from jax.experimental.pallas import tpu as pltpu
from jax.sharding import PartitionSpec as P

ITERS = 4
EPSILON = 1e-06
VMEM = pltpu.VMEM
SMEM = pltpu.SMEM


def peer(me, k, n):
    if n & (n - 1) == 0:
        return me ^ k, me ^ k
    return lax.rem(me + k, n), lax.rem(me + n - k, n)


def pairs(k, n):
    if n & (n - 1) == 0:
        return [(i, i ^ k) for i in range(n)]
    return [(i, (i + k) % n) for i in range(n)]


def roles(nb_ref, per):
    me = lax.axis_index("narrow")
    first = jnp.where(lax.div(nb_ref[0, 1], per) == me, 1, 0)
    last = 1 - first
    dev_prev = lax.div(nb_ref[first, 1], per)
    dev_next = lax.div(nb_ref[last, 2], per)
    return me, first, last, dev_prev, dev_next


def iota(shape, dim):
    return lax.broadcasted_iota(jnp.int32, shape, dim)


def pack(tile):
    w = tile.shape[0]
    h = w // 2
    top, low = tile[:h], tile[h:]
    low_left = jnp.concatenate([low[:, h:], low[:, :h]], axis=1)
    rows, cols = iota((h, w), 0), iota((h, w), 1)
    body = jnp.where(cols < rows, low_left, top)
    diag = jnp.sum(jnp.where(cols == rows, low_left, 0.0), axis=0, keepdims=True)
    return body, jnp.broadcast_to(diag, (8, w))


def unpack(body, diag):
    h, w = body.shape
    rows, cols = iota((h, w), 0), iota((h, w), 1)
    flipped = body.T
    mirror = jnp.concatenate([flipped[:h], flipped[:h]], axis=1)
    top = jnp.where(cols < rows, mirror, body)
    swapped = jnp.concatenate([body[:, h:], body[:, :h]], axis=1)
    col_low = cols - h
    right = jnp.where(col_low < rows, swapped, mirror)
    diag_right = jnp.concatenate([diag[:1, h:], diag[:1, :h]], axis=1)
    right = jnp.where(col_low == rows, jnp.broadcast_to(diag_right, (h, w)), right)
    low = jnp.where(cols < h, jnp.concatenate([flipped[h:], flipped[h:]], axis=1), right)
    return jnp.concatenate([top, low], axis=0)


def pack_kernel(n, nb_ref, h_ref, *out_refs):
    per, _, w, _ = h_ref.shape
    me, first, last, dev_prev, _ = roles(nb_ref, per)
    h = w // 2
    bodies, diags = zip(*[pack(h_ref[b, 0]) for b in range(per)])
    for k in range(1, n):
        to, _ = peer(me, k, n)
        chosen = jnp.where(dev_prev == to, first, last)
        out_refs[k - 1][:h] = jnp.where(chosen == 0, bodies[0], bodies[1])
        out_refs[k - 1][h:] = jnp.where(chosen == 0, diags[0], diags[1])


def split(x):
    high = x.astype(jnp.bfloat16)
    low = (x - high.astype(jnp.float32)).astype(jnp.bfloat16)
    return high, low


def dot(a, b):
    return jnp.dot(a, b, preferred_element_type=jnp.float32)


def product(a, b):
    ah, al = a
    bh, bl = b
    return dot(
        jnp.concatenate([ah, ah, al], axis=1), jnp.concatenate([bh, bl, bh], axis=0)
    )


def start_matrix(onsite, near, far, near_onsite, far_onsite, level):
    w = onsite.shape[0]
    zero = jnp.zeros((w, w), jnp.float32)
    matrix = jnp.concatenate(
        [
            jnp.concatenate([onsite, near, far], axis=1),
            jnp.concatenate([near.T, near_onsite, zero], axis=1),
            jnp.concatenate([far.T, zero, far_onsite], axis=1),
        ],
        axis=0,
    )
    order = matrix.shape[0]
    eye = jnp.where(iota((order, order), 0) == iota((order, order), 1), 1.0, 0.0)
    matrix = matrix - level * eye
    rows = jnp.sum(jnp.abs(matrix), axis=1, keepdims=True)
    bound = jnp.max(rows, axis=0, keepdims=True) + EPSILON
    return matrix * (1.0 / bound), eye


def main_kernel(n, nb_ref, live_ref, pot_ref, h_ref, old_ref, *refs):
    got, (dens_ref, half_ref), out_refs = refs[: n - 1], refs[n - 1 : n + 1], refs[n + 1 :]
    per, _, w, _ = h_ref.shape
    h = w // 2
    me, first, last, dev_prev, dev_next = roles(nb_ref, per)
    level = pot_ref[0]

    def received(source):
        body, diag = got[0][:h], got[0][h:]
        for k in range(2, n):
            _, origin = peer(me, k, n)
            body = jnp.where(origin == source, got[k - 1][:h], body)
            diag = jnp.where(origin == source, got[k - 1][h:], diag)
        return unpack(body, diag)

    from_prev, from_next = received(dev_prev), received(dev_next)
    blocks = []
    for own, other, near, far, remote in (
        (first, last, 2, 1, from_prev),
        (last, first, 1, 2, from_next),
    ):
        x, eye = start_matrix(
            h_ref[own, 0], h_ref[own, near], h_ref[own, far], h_ref[other, 0], remote, level
        )
        blocks.append(x)
    for sweep in range(ITERS - 1):
        for i in range(2):
            x = split(blocks[i])
            square = product(x, x)
            blocks[i] = product(x, split(1.5 * eye - 0.5 * square))
    fresh = []
    for i, (own, near, far) in enumerate(((first, 2, 1), (last, 1, 2))):
        xh, xl = split(blocks[i])
        square = product((xh, xl), (xh[:, :w], xl[:, :w]))
        cols = product((xh, xl), split(1.5 * eye[:, :w] - 0.5 * square))
        cols = 0.5 * (eye[:, :w] - cols)
        alive = live_ref[own] == 1
        fresh.append(
            [
                jnp.where(alive, cols[r * w : (r + 1) * w], old_ref[own, slot])
                for r, slot in enumerate((0, near, far))
            ]
        )
    (f0, f_near, f_far), (l0, l_near, l_far) = fresh
    half_ref[0] = 0.5 * f_far
    half_ref[1] = 0.5 * l_far
    f_send, l_send = (0.5 * f_far).T, (0.5 * l_far).T
    for k in range(1, n):
        to, _ = peer(me, k, n)
        out_refs[k - 1][...] = jnp.where(dev_prev == to, f_send, l_send)
    dens_ref[first, 0] = 0.5 * (f0 + f0.T)
    dens_ref[last, 0] = 0.5 * (l0 + l0.T)
    edge = 0.5 * (f_near + l_near.T)
    dens_ref[first, 2] = edge
    dens_ref[last, 1] = edge.T
    dens_ref[first, 1] = jnp.zeros_like(edge)
    dens_ref[last, 2] = jnp.zeros_like(edge)


def final_kernel(n, nb_ref, half_ref, dens_in, *refs):
    got, dens_ref, buf, sems = refs[: n - 1], refs[n - 1], refs[n], refs[n + 1]
    me, first, last, dev_prev, dev_next = roles(nb_ref, 2)

    def received(source):
        tile = got[0][...]
        for k in range(2, n):
            _, origin = peer(me, k, n)
            tile = jnp.where(origin == source, got[k - 1][...], tile)
        return tile

    buf[0] = half_ref[0] + received(dev_prev)
    one = pltpu.make_async_copy(buf.at[0], dens_ref.at[first, 1], sems.at[0])
    one.start()
    buf[1] = half_ref[1] + received(dev_next)
    two = pltpu.make_async_copy(buf.at[1], dens_ref.at[last, 2], sems.at[1])
    two.start()
    one.wait()
    two.wait()


def vspec():
    return pl.BlockSpec(memory_space=VMEM)


def sspec():
    return pl.BlockSpec(memory_space=SMEM)


def shards(n, hamiltonian, old_density, neighbours, live, potential):
    per, _, w, _ = hamiltonian.shape
    assert per == 2 and n > 2
    f32 = jnp.float32
    diag_msgs = pl.pallas_call(
        functools.partial(pack_kernel, n),
        out_shape=[jax.ShapeDtypeStruct((w // 2 + 8, w), f32)] * (n - 1),
        grid=(1,),
        in_specs=[sspec(), pl.BlockSpec((per, 1, w, w), lambda i: (0, 0, 0, 0))],
        out_specs=[vspec()] * (n - 1),
    )(neighbours, hamiltonian)
    got = [lax.ppermute(m, "narrow", pairs(k + 1, n)) for k, m in enumerate(diag_msgs)]
    dens, half, *tiles = pl.pallas_call(
        functools.partial(main_kernel, n),
        out_shape=[
            jax.ShapeDtypeStruct(hamiltonian.shape, f32),
            jax.ShapeDtypeStruct((2, w, w), f32),
        ]
        + [jax.ShapeDtypeStruct((w, w), f32)] * (n - 1),
        in_specs=[sspec()] * 3 + [vspec()] * (n + 1),
        out_specs=[vspec()] * (n + 1),
    )(neighbours, live, potential, hamiltonian, old_density, *got)
    back = [lax.ppermute(m, "narrow", pairs(k + 1, n)) for k, m in enumerate(tiles)]
    return pl.pallas_call(
        functools.partial(final_kernel, n),
        out_shape=jax.ShapeDtypeStruct(hamiltonian.shape, f32),
        in_specs=[sspec(), vspec(), pl.BlockSpec(memory_space=pl.ANY)] + [vspec()] * (n - 1),
        out_specs=pl.BlockSpec(memory_space=pl.ANY),
        scratch_shapes=[pltpu.VMEM((2, w, w), f32), pltpu.SemaphoreType.DMA((2,))],
        input_output_aliases={2: 0},
    )(neighbours, half, dens, *back)


def solution(mesh):
    placed = (
        P(("wide", "narrow"), None, None, None),
        P(("wide", "narrow"), None, None, None),
        P(("wide", "narrow"), None),
        P(("wide", "narrow")),
        P(),
    )
    return jax.shard_map(
        functools.partial(shards, mesh.shape["narrow"]),
        mesh=mesh,
        in_specs=placed,
        out_specs=P(("wide", "narrow"), None, None, None),
        check_vma=False,
    )
```
